128 devices in a mesh: mp: 32 (over y, x, core), ffn: 4 (over z).
Axes of the slice: x: 4, y: 4, z: 4, core: 2. Of those that a mesh axis runs over, the one named last changes fastest.
Arguments:
- tokens: bfloat16 [512, 8192], P('ffn', 'mp'), may hold values from -6 to 6
- gate_weight: bfloat16 [8192, 28672], P('mp', 'ffn'), may hold values from -0.0625 to 0.0625
- up_weight: bfloat16 [8192, 28672], P('mp', 'ffn'), may hold values from -0.0625 to 0.0625
- down_weight: bfloat16 [28672, 8192], P('ffn', 'mp'), may hold values from -0.03125 to 0.03125
Outputs:
- mixed: bfloat16 [512, 8192], P('ffn', 'mp')
The draws below stay inside these ranges and needn't reach their ends.
All inputs are finite; a program needn't handle non-finite values.
Results may differ from the reference program's by a relative error of at most 0.005.
Values may be sent and summed in bfloat16 or wider, within the bound.
A program may use at most 192 MiB of HBM per device.

```python
import jax
import jax.numpy as jnp

D = 8192
FF = 28672
BATCH = 512


def steps_of(rng, shape, pieces, low, top_value):
    gain = 1.0
    for position, parts in pieces:
        draws = jax.random.uniform(jax.random.fold_in(jax.random.fold_in(rng, 6), position), (parts,), jnp.float32, low / len(pieces), top_value / len(pieces))
        gain = gain * jnp.repeat(jnp.exp(draws), shape[position] // parts).reshape((-1,) + (1,) * (len(shape) - 1 - position))
    return gain


def scatter_about(rng, shape, scale, reach, shards=(), dtype=jnp.bfloat16):
    gain = steps_of(rng, shape, shards, -0.22, 0.18) if shards else 1.0
    values = jax.random.normal(rng, shape, jnp.float32) * scale * gain
    return jnp.minimum(jnp.maximum(values, -reach), reach).astype(dtype)


def setup_inputs(seed: int = 0) -> dict:
    arg_keys = jax.random.split(jax.random.key(seed), 5)
    tokens = scatter_about(arg_keys[0], (BATCH, D), 1.0, 6.0, ((0, 4), (1, 32)))
    gate_weight = scatter_about(arg_keys[1], (D, FF), D ** -0.5, 0.0625, ((0, 32), (1, 4)))
    up_weight = scatter_about(arg_keys[2], (D, FF), D ** -0.5, 0.0625, ((0, 32), (1, 4)))
    down_weight = scatter_about(arg_keys[3], (FF, D), FF ** -0.5, 0.03125, ((0, 4), (1, 32)))
    return dict(tokens=tokens, gate_weight=gate_weight, up_weight=up_weight, down_weight=down_weight)


def reference(tokens, gate_weight, up_weight, down_weight):
    gate = jnp.dot(tokens, gate_weight, preferred_element_type=jnp.float32)
    up = jnp.dot(tokens, up_weight, preferred_element_type=jnp.float32)
    hidden = (jax.nn.silu(gate) * up).astype(jnp.bfloat16)
    mixed = jnp.dot(hidden, down_weight, preferred_element_type=jnp.float32)
    return mixed.astype(jnp.bfloat16)
```

```python
import jax
import jax.numpy as jnp
from jax import lax
from jax.experimental import pallas as pl
from jax.experimental.pallas import tpu as pltpu
from jax.sharding import PartitionSpec as P

MESH = pl.DeviceIdType.MESH
CLASSES = 4
SUBS = 2
F32 = jnp.float32
BF16 = jnp.bfloat16


def coded(v):
    return (v * jnp.abs(v)).astype(BF16)


def decoded(c):
    u = c.astype(F32)
    return u * lax.rsqrt(jnp.maximum(jnp.abs(u), 1e-37))


def kernel(
    tokens, gate, up, down, out,
    w, dw, x, s1, r1, k1, s2, r2, k2, s3, r3, k3, s4, r4, k4, h, od, rd, t, zr,
    ssem, rsem, load_sem, tok_send, tok_recv, w_send, w_recv, end_send, end_recv,
):
    rows, depth = tokens.shape
    units = w.shape[2]
    half, quarter = units // 2, units // 4
    sub = rows // SUBS
    me = lax.axis_index("mp")
    z = lax.axis_index("ffn")
    core = lax.rem(me, 2)
    xpos = lax.rem(lax.div(me, 2), 4)
    ypos = lax.div(me, 8)
    sib = 1 - core
    sibling = me + 1 - 2 * core

    def dim_of(q, stage):
        return lax.rem(q + stage, 4)

    def bit_of(q, stage):
        d = dim_of(q, stage)
        is_y, is_b = lax.rem(d, 2), lax.div(d, 2)
        pos = xpos * (1 - is_y) + ypos * is_y
        return lax.rem(lax.div(pos + 1, 2), 2) * (1 - is_b) + lax.div(pos, 2) * is_b

    def peer_of(q, stage):
        d = dim_of(q, stage)
        is_y, is_b = lax.rem(d, 2), lax.div(d, 2)
        pos = xpos * (1 - is_y) + ypos * is_y
        to_a = pos + 1 - 2 * lax.rem(pos, 2)
        to_b = lax.rem(pos + 1 + 2 * lax.rem(pos + 1, 2), 4)
        shift = to_a * (1 - is_b) + to_b * is_b - pos
        return me + 2 * shift * (1 - is_y) + 8 * shift * is_y

    def remote(src, dst, send, recv, mp, ffn):
        return pltpu.make_async_remote_copy(
            src_ref=src, dst_ref=dst, send_sem=send, recv_sem=recv,
            device_id={"mp": mp, "ffn": ffn}, device_id_type=MESH,
        )

    def lanes(start, size):
        return pl.ds(pl.multiple_of(start, 128), size)

    def sublanes(start, size):
        return pl.ds(pl.multiple_of(start, 16), size)

    def each_class(body):
        def step(j, carry):
            body(j, lax.rem(z + j, 4))
            return carry

        lax.fori_loop(0, CLASSES, step, 0)

    mine = lanes(core * depth, depth)
    loads = [
        pltpu.make_async_copy(tokens, x.at[z, :, mine], load_sem.at[0]),
        pltpu.make_async_copy(
            gate.at[:, lanes(core * units, units)],
            w.at[0, sublanes(core * depth, depth), :], load_sem.at[1]),
        pltpu.make_async_copy(
            up.at[:, lanes(core * units, units)],
            w.at[1, sublanes(core * depth, depth), :], load_sem.at[2]),
        pltpu.make_async_copy(
            down.at[sublanes(core * units, units), :], dw.at[:, mine], load_sem.at[3]),
    ]
    for load in loads:
        load.start()

    barrier = pltpu.get_barrier_semaphore()
    peers = [(sibling, z)]
    peers += [(peer_of(0, d), z) for d in range(4)]
    peers += [(me, lax.rem(z + j, 4)) for j in range(1, 4)]
    for mp, ffn in peers:
        pl.semaphore_signal(barrier, inc=1, device_id={"mp": mp, "ffn": ffn}, device_id_type=MESH)
    pl.semaphore_wait(barrier, len(peers))

    def token_copy(j):
        to = lax.rem(z + j, 4)
        return remote(tokens, x.at[z, :, mine], tok_send.at[j], tok_recv.at[4 - j], me, to)

    def relay_copy(j):
        q = lax.rem(z + j, 4)
        src = tokens if j == 0 else x.at[q, :, mine]
        return remote(src, x.at[q, :, mine], tok_send.at[4 + j], tok_recv.at[4 + j], sibling, z)

    for j in range(1, 4):
        token_copy(j).start()
    relay_copy(0).start()

    first_half = 1 - bit_of(z, 0)

    def weight_copy(chunk, m):
        which = first_half if chunk == 0 else 1 - first_half
        src = (gate, up)[m].at[:, lanes(sib * units + which * half, half)]
        dst = w.at[m, sublanes(core * depth, depth), lanes(which * half, half)]
        return remote(src, dst, w_send.at[2 * chunk + m], w_recv.at[2 * chunk + m], sibling, z)

    down_copy = remote(
        down.at[sublanes(sib * units, units), :], dw.at[:, mine],
        w_send.at[4], w_recv.at[4], sibling, z)
    for chunk in range(2):
        for m in range(2):
            weight_copy(chunk, m).start()

    for j in range(1, 4):
        token_copy(4 - j).wait_recv()
        relay_copy(j).start()
    for load in loads[:3]:
        load.wait()
    for j in range(4):
        relay_copy(j).wait_recv()

    def stage_copy(stage, q, s):
        src, dst = ((s1, r1), (s2, r2), (s3, r3), (s4, r4))[stage]
        return remote(
            src.at[q, s], dst.at[q, s], ssem.at[stage, 2 * q + s], rsem.at[stage, 2 * q + s],
            peer_of(q, stage), z)

    for m in range(2):
        weight_copy(0, m).wait_recv()

    def first(j, q):
        @pl.when(j == 1)
        def _():
            for m in range(2):
                weight_copy(1, m).wait_recv()

        other = lanes((1 - bit_of(q, 0)) * half, half)
        for m in range(2):
            part = jnp.dot(x[q], w[m, :, other], preferred_element_type=F32)
            for s in range(SUBS):
                s1[q, s, m] = coded(part[s * sub : (s + 1) * sub])
        for s in range(SUBS):
            stage_copy(0, q, s).start()

    each_class(first)
    down_copy.start()

    def kept(j, q):
        own = lanes(bit_of(q, 0) * half, half)
        for m in range(2):
            part = jnp.dot(x[q], w[m, :, own], preferred_element_type=F32)
            for s in range(SUBS):
                k1[q, s, m] = part[s * sub : (s + 1) * sub]

    each_class(kept)

    def by_rows(count, body):
        def step(i, carry):
            body(lax.div(i, count), sublanes(lax.rem(i, count) * 16, 16), lax.rem(i, count) * 16)
            return carry

        lax.fori_loop(0, 2 * count, step, 0)

    def columns_step(s):
        def send(j, q):
            stage_copy(0, q, s).wait_recv()
            cols = lanes((1 - bit_of(q, 1)) * quarter, quarter)

            def body(m, rs, _):
                s2[q, s, m, rs, :] = coded(k1[q, s, m, rs, cols] + decoded(r1[q, s, m, rs, cols]))

            by_rows(sub // 16, body)
            stage_copy(1, q, s).start()

        def keep(j, q):
            cols = lanes(bit_of(q, 1) * quarter, quarter)

            def body(m, rs, _):
                k2[q, s, m, rs, :] = k1[q, s, m, rs, cols] + decoded(r1[q, s, m, rs, cols])

            by_rows(sub // 16, body)

        each_class(send)
        each_class(keep)

    def rows_step(stage, s, k, r, out_s, out_k):
        size = out_s.shape[3]

        def send(j, q):
            stage_copy(stage - 1, q, s).wait_recv()
            base = (1 - bit_of(q, stage)) * size

            def body(m, rs, at):
                here = sublanes(base + at, 16)
                out_s[q, s, m, rs, :] = coded(k[q, s, m, here, :] + decoded(r[q, s, m, here, :]))

            by_rows(size // 16, body)
            stage_copy(stage, q, s).start()

        def keep(j, q):
            base = bit_of(q, stage) * size

            def body(m, rs, at):
                here = sublanes(base + at, 16)
                out_k[q, s, m, rs, :] = k[q, s, m, here, :] + decoded(r[q, s, m, here, :])

            by_rows(size // 16, body)

        each_class(send)
        each_class(keep)

    def gather_copy(step, q, s):
        stage = 3 - step
        row, col = q * sub, bit_of(q, 0) * half
        if step < 3:
            col += bit_of(q, 1) * quarter
        if step < 2:
            row += bit_of(q, 2) * (sub // 2)
        if step < 1:
            row += bit_of(q, 3) * (sub // 4)
        n_rows = (sub // 4, sub // 2, sub, sub)[step]
        n_cols = half if step == 3 else quarter
        block = h.at[s, sublanes(row, n_rows), lanes(col, n_cols)]
        sem = 4 + step
        return remote(
            block, block, ssem.at[sem, 2 * q + s], rsem.at[sem, 2 * q + s], peer_of(q, stage), z)

    def hidden_step(s):
        def body(j, q):
            stage_copy(3, q, s).wait_recv()
            g = k4[q, s, 0] + decoded(r4[q, s, 0])
            u = k4[q, s, 1] + decoded(r4[q, s, 1])
            row = q * sub + bit_of(q, 2) * (sub // 2) + bit_of(q, 3) * (sub // 4)
            col = bit_of(q, 0) * half + bit_of(q, 1) * quarter
            value = g / (1.0 + jnp.exp(-g)) * u
            h[s, sublanes(row, sub // 4), lanes(col, quarter)] = value.astype(BF16)
            gather_copy(0, q, s).start()

        each_class(body)

    def gather_step(step, s):
        def body(j, q):
            gather_copy(step - 1, q, s).wait_recv()
            gather_copy(step, q, s).start()

        each_class(body)

    for s in range(SUBS):
        columns_step(s)
    for s in range(SUBS):
        rows_step(2, s, k2, r2, s3, k3)
    for s in range(SUBS):
        rows_step(3, s, k3, r3, s4, k4)
    for s in range(SUBS):
        hidden_step(s)
    for step in range(1, 4):
        for s in range(SUBS):
            gather_step(step, s)

    loads[3].wait()
    down_copy.wait_recv()

    def swap_copy(s):
        return remote(od.at[s], rd.at[s], end_send.at[s, 0], end_recv.at[s, 0], sibling, z)

    def owner_copy(s, j):
        q = lax.rem(z + j, 4)
        src = t.at[s, sublanes(q * sub, sub), :]
        return remote(src, zr.at[s, 3 - j], end_send.at[s, j], end_recv.at[s, 4 - j], me, q)

    def project(s):
        def body(j, q):
            gather_copy(3, q, s).wait_recv()

        each_class(body)
        theirs = lanes(sib * depth, depth)
        od[s] = jnp.dot(h[s], dw[:, theirs], preferred_element_type=F32)
        swap_copy(s).start()
        t[s] = jnp.dot(h[s], dw[:, mine], preferred_element_type=F32)
        swap_copy(s).wait_recv()
        t[s] += rd[s]
        for j in range(1, 4):
            owner_copy(s, j).start()

    for s in range(SUBS):
        project(s)
    for s in range(SUBS):
        for j in range(1, 4):
            owner_copy(s, j).wait_recv()
        total = t[s, sublanes(z * sub, sub), :]
        for j in range(3):
            total += zr[s, j]
        out[pl.ds(s * sub, sub), :] = total.astype(BF16)

    for j in range(1, 4):
        token_copy(j).wait_send()
    for j in range(4):
        relay_copy(j).wait_send()
    for chunk in range(2):
        for m in range(2):
            weight_copy(chunk, m).wait_send()
    down_copy.wait_send()

    def drain(j, q):
        for s in range(SUBS):
            for stage in range(4):
                stage_copy(stage, q, s).wait_send()
                gather_copy(stage, q, s).wait_send()

    each_class(drain)
    for s in range(SUBS):
        swap_copy(s).wait_send()
        for j in range(1, 4):
            owner_copy(s, j).wait_send()


def local(tokens, gate, up, down):
    rows, depth = tokens.shape
    units = gate.shape[1] // 2
    sub = rows // SUBS
    lead = (CLASSES, SUBS, 2)

    def pieces(n_rows, n_cols):
        shape = (*lead, n_rows, n_cols)
        return [pltpu.VMEM(shape, BF16), pltpu.VMEM(shape, BF16), pltpu.VMEM(shape, F32)]

    sem = pltpu.SemaphoreType.DMA
    return pl.pallas_call(
        kernel,
        out_shape=jax.ShapeDtypeStruct((rows, depth), BF16),
        in_specs=[pl.BlockSpec(memory_space=pl.ANY)] * 4,
        out_specs=pl.BlockSpec(memory_space=pltpu.VMEM),
        scratch_shapes=[
            pltpu.VMEM((2, 2 * depth, units), BF16),
            pltpu.VMEM((units, 2 * depth), BF16),
            pltpu.VMEM((CLASSES, rows, 2 * depth), BF16),
            *pieces(sub, units // 2),
            *pieces(sub, units // 4),
            *pieces(sub // 2, units // 4),
            *pieces(sub // 4, units // 4),
            pltpu.VMEM((SUBS, CLASSES * sub, units), BF16),
            pltpu.VMEM((SUBS, CLASSES * sub, depth), F32),
            pltpu.VMEM((SUBS, CLASSES * sub, depth), F32),
            pltpu.VMEM((SUBS, CLASSES * sub, depth), F32),
            pltpu.VMEM((SUBS, 3, sub, depth), F32),
            sem((8, CLASSES * SUBS)),
            sem((8, CLASSES * SUBS)),
            sem((4,)),
            sem((8,)),
            sem((8,)),
            sem((5,)),
            sem((5,)),
            sem((SUBS, 4)),
            sem((SUBS, 4)),
        ],
        compiler_params=pltpu.CompilerParams(
            collective_id=0, has_side_effects=True, vmem_limit_bytes=60 * 2**20
        ),
    )(tokens, gate, up, down)


def solution(mesh):
    placed = (P("ffn", "mp"), P("mp", "ffn"), P("mp", "ffn"), P("ffn", "mp"))
    return jax.shard_map(
        local, mesh=mesh, in_specs=placed, out_specs=P("ffn", "mp"), check_vma=False
    )
```

```python
import jax
import jax.numpy as jnp
from jax import lax
from jax.experimental import pallas as pl
from jax.experimental.pallas import tpu as pltpu
from jax.sharding import PartitionSpec as P

MESH = pl.DeviceIdType.MESH
STREAMS = 4
LINKS = 4
ORDERS = ((0, 1, 3, 2), (1, 3, 2, 0), (1, 2, 3, 0), (2, 1, 3, 0))
F32 = jnp.float32
BF16 = jnp.bfloat16


def coded(v):
    return (v * jnp.abs(v)).astype(BF16)


def decoded(c):
    u = c.astype(F32)
    return u * lax.rsqrt(jnp.maximum(jnp.abs(u), 1e-37))


def kernel(
    tokens, gate, up, down, out,
    w, ws, dw, x, p, s1, r1, s2, r2, k2, s3, r3, k3, s4, r4, h, od, rd, t, tc, zr,
    ssem, rsem0, rsem, load_sem, tok_sem, relay_sem, w_sem, swap_sem, own_sem,
):
    rows, depth = tokens.shape
    units = w.shape[2]
    half, quarter = units // 2, units // 4
    sub = rows // LINKS
    part = sub // 2
    me = lax.axis_index("mp")
    z = lax.axis_index("ffn")
    core = lax.rem(me, 2)
    xpos = lax.rem(lax.div(me, 2), 4)
    ypos = lax.div(me, 8)
    sib = 1 - core
    sibling = me + 1 - 2 * core

    bits, peers = [], []
    for pos, stride in ((xpos, 2), (ypos, 8)):
        bits.append(lax.rem(lax.div(pos + 1, 2), 2))
        peers.append(me + stride * (1 - 2 * lax.rem(pos, 2)))
    for pos, stride in ((xpos, 2), (ypos, 8)):
        bits.append(lax.div(pos, 2))
        peers.append(me + stride * (lax.rem(pos + 1 + 2 * lax.rem(pos + 1, 2), 4) - pos))

    def bit(s, stage):
        return bits[(s + stage) % 4]

    def peer(s, stage):
        return peers[(s + stage) % 4]

    def along_z(j):
        return lax.rem(z + j, 4)

    def remote(src, dst, send, recv, mp, ffn):
        return pltpu.make_async_remote_copy(
            src_ref=src, dst_ref=dst, send_sem=send, recv_sem=recv,
            device_id={"mp": mp, "ffn": ffn}, device_id_type=MESH,
        )

    def lanes(start, size):
        return pl.ds(pl.multiple_of(start, 128), size)

    def sublanes(start, size):
        return pl.ds(pl.multiple_of(start, 16), size)

    mine, theirs = lanes(core * depth, depth), lanes(sib * depth, depth)
    my_rows = sublanes(core * depth, depth)

    pieces = [(0, 0), (1, 0), (0, 1), (1, 1)]
    token_load = pltpu.make_async_copy(tokens, x.at[0, :, mine], load_sem.at[0])
    token_load.start()
    stage_loads = []
    for i, (a, e) in enumerate(pieces):
        cols = pl.ds(a * half + e * quarter, quarter)
        from_cols = lanes(sib * units + a * half + e * quarter, quarter)
        for m, ref in enumerate((gate, up)):
            stage_loads.append(
                pltpu.make_async_copy(ref.at[:, from_cols], ws.at[m, :, cols], load_sem.at[1 + 2 * i + m]))
            stage_loads[-1].start()
        if i == 0:
            own_loads = []
            for m, ref in enumerate((gate, up)):
                own_loads.append(pltpu.make_async_copy(
                    ref.at[:, lanes(core * units, units)], w.at[m, my_rows, :], load_sem.at[9 + m]))
                own_loads[-1].start()
    down_load = pltpu.make_async_copy(
        down.at[sublanes(core * units, units), :], dw.at[:, mine], load_sem.at[11])
    down_load.start()

    barrier = pltpu.get_barrier_semaphore()
    partners = [(sibling, z)] + [(q, z) for q in peers] + [(me, along_z(j)) for j in range(1, 4)]
    for mp, ffn in partners:
        pl.semaphore_signal(barrier, inc=1, device_id={"mp": mp, "ffn": ffn}, device_id_type=MESH)
    with jax.named_scope("z_barrier"):
        pl.semaphore_wait(barrier, len(partners))

    def token_copy(j):
        return remote(
            x.at[0, :, mine], x.at[4 - j, :, mine], tok_sem.at[0, j], tok_sem.at[1, 4 - j], me, along_z(j))

    def relay_copy(j):
        block = x.at[j, :, mine]
        return remote(block, block, relay_sem.at[0, j], relay_sem.at[1, j], sibling, z)

    def weight_copy(i):
        a, e = pieces[i]
        cols = pl.ds(a * half + e * quarter, quarter)
        return remote(ws.at[:, :, cols], w.at[:, my_rows, cols], w_sem.at[0, i], w_sem.at[1, i], sibling, z)

    down_copy = remote(
        down.at[sublanes(sib * units, units), :], dw.at[:, mine], w_sem.at[0, 4], w_sem.at[1, 4], sibling, z)

    def send_weights(i):
        stage_loads[2 * i].wait()
        stage_loads[2 * i + 1].wait()
        weight_copy(i).start()

    token_load.wait()
    for j in (1, 3, 2):
        token_copy(j).start()
    relay_copy(0).start()
    send_weights(0)
    send_weights(1)

    def partial(j, i):
        a, e = pieces[i]
        cols = pl.ds(a * half + e * quarter, quarter)
        for m in range(2):
            p[j, 2 * a + e, m] = jnp.dot(x[j], w[m, :, cols], preferred_element_type=F32)

    def by_rows(count, body):
        def step(i, carry):
            body(lax.div(i, count), lax.rem(i, count) * 16)
            return carry

        lax.fori_loop(0, 2 * count, step, 0)

    def first_copy(j, e, s):
        rs = pl.ds(s * sub, sub)
        return remote(
            s1.at[j, e, :, rs, :], r1.at[j, e, :, rs, :], ssem.at[0], rsem0.at[j, 4 * e + s], peer(s, 0), z)

    def first(j, e):
        for s in range(LINKS):

            def body(m, at, s=s):
                rs = sublanes(s * sub + at, 16)
                s1[j, e, m, rs, :] = coded(p[j, 2 * (1 - bit(s, 0)) + e, m, rs, :])

            by_rows(sub // 16, body)
            first_copy(j, e, s).start()

    with jax.named_scope("z_load"):
        for load in own_loads:
            load.wait()
        relay_copy(0).wait_recv()
    with jax.named_scope("z_w0"):
        weight_copy(0).wait_recv()
    partial(0, 0)
    with jax.named_scope("z_tok"):
        for j in (1, 3):
            token_copy(4 - j).wait_recv()
            relay_copy(j).start()
    send_weights(2)
    with jax.named_scope("z_w1"):
        weight_copy(1).wait_recv()
    with jax.named_scope("z_f00"):
        partial(0, 1)
        first(0, 0)
    with jax.named_scope("z_rel1"):
        relay_copy(1).wait_recv()
    with jax.named_scope("z_f10"):
        partial(1, 0)
        partial(1, 1)
        first(1, 0)
    with jax.named_scope("z_tok2"):
        token_copy(2).wait_recv()
        relay_copy(2).start()
    send_weights(3)
    with jax.named_scope("z_w23"):
        weight_copy(2).wait_recv()
        partial(0, 2)
        partial(1, 2)
        weight_copy(3).wait_recv()
    with jax.named_scope("z_f01"):
        for j in (0, 1):
            partial(j, 3)
            first(j, 1)
    for j in (3, 2):
        with jax.named_scope("z_f%d" % j):
            relay_copy(j).wait_recv()
            for e in range(2):
                partial(j, 2 * e)
                partial(j, 2 * e + 1)
                first(j, e)
    down_copy.start()

    def second_copy(j, s):
        rs = pl.ds(s * sub, sub)
        return remote(s2.at[j, :, rs, :], r2.at[j, :, rs, :], ssem.at[1], rsem.at[0, j, s], peer(s, 1), z)

    def second(j):
        def add(dst, s, e, done):
            def body(m, at):
                rs = sublanes(s * sub + at, 16)
                dst[j, m, rs, :] = done(p[j, 2 * bit(s, 0) + e, m, rs, :] + decoded(r1[j, e, m, rs, :]))

            by_rows(sub // 16, body)

        for s in range(LINKS):
            for e in range(2):
                first_copy(j, e, s).wait_recv()
            add(s2, s, 1 - bit(s, 1), coded)
            second_copy(j, s).start()
        for s in range(LINKS):
            add(k2, s, bit(s, 1), lambda v: v)

    def third_copy(j, s):
        rs = pl.ds(s * part, part)
        return remote(s3.at[j, :, rs, :], r3.at[j, :, rs, :], ssem.at[2], rsem.at[1, j, s], peer(s, 2), z)

    def third(j):
        def add(dst, s, side, done):
            def body(m, at):
                rs = sublanes(s * part + at, 16)
                src = sublanes(s * sub + side * part + at, 16)
                dst[j, m, rs, :] = done(k2[j, m, src, :] + decoded(r2[j, m, src, :]))

            by_rows(part // 16, body)

        for s in range(LINKS):
            second_copy(j, s).wait_recv()
            add(s3, s, 1 - bit(s, 2), coded)
            third_copy(j, s).start()
        for s in range(LINKS):
            add(k3, s, bit(s, 2), lambda v: v)

    def fourth_copy(j, s):
        rs = pl.ds(s * part, part)
        return remote(s4.at[j, :, rs, :], r4.at[j, :, rs, :], ssem.at[3], rsem.at[2, j, s], peer(s, 3), z)

    def fourth(j):
        for s in range(LINKS):
            third_copy(j, s).wait_recv()

            def body(m, at, s=s):
                rs = sublanes(s * part + at, 16)
                v = k3[j, m, rs, :] + decoded(r3[j, m, rs, :])
                k3[j, m, rs, :] = v
                s4[j, m, rs, :] = coded(v)

            by_rows(part // 16, body)
            fourth_copy(j, s).start()

    def gather_copy(step, j, s):
        row, col = s * sub, bit(s, 0) * half
        n_rows, n_cols = sub, half
        if step < 2:
            col, n_cols = col + bit(s, 1) * quarter, quarter
        if step < 1:
            row, n_rows = row + bit(s, 2) * part, part
        block = h.at[j, sublanes(row, n_rows), lanes(col, n_cols)]
        return remote(block, block, ssem.at[4 + step], rsem.at[3 + step, j, s], peer(s, 2 - step), z)

    def hidden(j):
        for s in range(LINKS):
            fourth_copy(j, s).wait_recv()
            row, cols = s * sub + bit(s, 2) * part, lanes(bit(s, 0) * half + bit(s, 1) * quarter, quarter)

            def body(i, carry, s=s, row=row, cols=cols):
                rs = sublanes(s * part + i * 16, 16)
                g = k3[j, 0, rs, :] + decoded(r4[j, 0, rs, :])
                u = k3[j, 1, rs, :] + decoded(r4[j, 1, rs, :])
                value = g / (1.0 + jnp.exp(-g)) * u
                h[j, sublanes(row + i * 16, 16), cols] = value.astype(BF16)
                return carry

            lax.fori_loop(0, part // 16, body, 0)
            gather_copy(0, j, s).start()

    def gather(step, j):
        for s in range(LINKS):
            gather_copy(step - 1, j, s).wait_recv()
            gather_copy(step, j, s).start()

    def phase(name, order, run):
        for j in order:
            with jax.named_scope("z_%s%d" % (name, j)):
                run(j)

    phase("second", ORDERS[1], second)
    phase("third", ORDERS[2], third)
    phase("fourth", ORDERS[3], fourth)
    phase("hidden", ORDERS[3], hidden)
    phase("ga", ORDERS[3], lambda j: gather(1, j))
    phase("gb", ORDERS[3], lambda j: gather(2, j))

    down_load.wait()
    down_copy.wait_recv()

    def swap_copy(j):
        return remote(od.at[j], rd.at[j], swap_sem.at[0, j], swap_sem.at[1, j], sibling, z)

    def owner_copy(j):
        return remote(tc.at[j], zr.at[3 - j], own_sem.at[0, j], own_sem.at[1, 4 - j], me, along_z(j))

    def project(j):
        with jax.named_scope("z_gc%d" % j):
            for s in range(LINKS):
                gather_copy(2, j, s).wait_recv()
        with jax.named_scope("z_dot%d" % j):
            od[j] = jnp.dot(h[j], dw[:, theirs], preferred_element_type=F32)
            swap_copy(j).start()
            t[j] = jnp.dot(h[j], dw[:, mine], preferred_element_type=F32)

    def to_owner(j):
        with jax.named_scope("z_swap%d" % j):
            swap_copy(j).wait_recv()
        tc[j] = coded(t[j] + rd[j])
        owner_copy(j).start()

    last = None
    for j in ORDERS[3]:
        project(j)
        if last is not None:
            to_owner(last)
        last = j

    for j in range(1, 4):
        token_copy(j).wait_send()
        owner_copy(j).wait_send()
    for j in range(4):
        relay_copy(j).wait_send()
        weight_copy(j).wait_send()
    down_copy.wait_send()
    everything = [s1, s2, s3, s4, h.at[0, pl.ds(0, rows // 2), :], h.at[0], h.at[pl.ds(0, 2)]]
    for i, sent in enumerate(everything):
        remote(sent, sent, ssem.at[i], rsem.at[0, 0, 0], sibling, z).wait_send()
    for j in range(4):
        swap_copy(j).wait_send()
    with jax.named_scope("z_swap0"):
        swap_copy(0).wait_recv()
    with jax.named_scope("z_own"):
        for j in range(1, 4):
            owner_copy(j).wait_recv()
    total = t[0] + rd[0]
    for j in range(3):
        total += decoded(zr[j])
    out[...] = total.astype(out.dtype)


def local(tokens, gate, up, down):
    rows, depth = tokens.shape
    units = gate.shape[1] // 2
    quarter = units // 4
    sem = pltpu.SemaphoreType.DMA
    tall, low = (STREAMS, 2, rows, quarter), (STREAMS, 2, rows // 2, quarter)
    result = (STREAMS, rows, depth)
    return pl.pallas_call(
        kernel,
        out_shape=jax.ShapeDtypeStruct((rows, depth), BF16),
        in_specs=[pl.BlockSpec(memory_space=pl.ANY)] * 4,
        out_specs=pl.BlockSpec(memory_space=pltpu.VMEM),
        scratch_shapes=[
            pltpu.VMEM((2, 2 * depth, units), BF16),
            pltpu.VMEM((2, depth, units), BF16),
            pltpu.VMEM((units, 2 * depth), BF16),
            pltpu.VMEM((STREAMS, rows, 2 * depth), BF16),
            pltpu.VMEM((STREAMS, 4, 2, rows, quarter), F32),
            *[pltpu.VMEM((STREAMS, 2, 2, rows, quarter), BF16) for _ in range(2)],
            *[pltpu.VMEM(tall, dtype) for dtype in (BF16, BF16, F32)],
            *[pltpu.VMEM(low, dtype) for dtype in (BF16, BF16, F32)],
            *[pltpu.VMEM(low, dtype) for dtype in (BF16, BF16)],
            pltpu.VMEM((STREAMS, rows, units), BF16),
            pltpu.VMEM(result, F32),
            pltpu.VMEM(result, F32),
            pltpu.VMEM(result, F32),
            pltpu.VMEM(result, BF16),
            pltpu.VMEM((3, rows, depth), BF16),
            sem((7,)),
            sem((STREAMS, 2 * LINKS)),
            sem((6, STREAMS, LINKS)),
            sem((12,)),
            sem((2, STREAMS)),
            sem((2, STREAMS)),
            sem((2, 5)),
            sem((2, STREAMS)),
            sem((2, STREAMS)),
        ],
        compiler_params=pltpu.CompilerParams(
            collective_id=0, has_side_effects=True, vmem_limit_bytes=60 * 2**20
        ),
    )(tokens, gate, up, down)


def solution(mesh):
    placed = (P("ffn", "mp"), P("mp", "ffn"), P("mp", "ffn"), P("ffn", "mp"))
    return jax.shard_map(
        local, mesh=mesh, in_specs=placed, out_specs=P("ffn", "mp"), check_vma=False
    )
```

```python
import jax
import jax.numpy as jnp
from jax import lax
from jax.experimental import pallas as pl
from jax.experimental.pallas import tpu as pltpu
from jax.sharding import PartitionSpec as P

MESH = pl.DeviceIdType.MESH
STREAMS = 4
LINKS = 4
ORDERS = ((0, 1, 3, 2), (1, 3, 2, 0), (1, 2, 3, 0), (2, 1, 3, 0))
F32 = jnp.float32
BF16 = jnp.bfloat16


def coded(v):
    return (v * jnp.abs(v)).astype(BF16)


def decoded(c):
    u = c.astype(F32)
    return u * lax.rsqrt(jnp.maximum(jnp.abs(u), 1e-37))


def kernel(
    tokens, gate, up, down, out,
    w, ws, dw, x, p, s1, r1, s2, r2, k2, s3, r3, k3, s4, r4, h, od, rd, t, tc, zr,
    sx, rx, ssem, rsem0, rsem, load_sem, tok_sem, relay_sem, w_sem, sx_sem, swap_sem, own_sem,
):
    rows, depth = tokens.shape
    units = w.shape[2]
    half, quarter = units // 2, units // 4
    sub = rows // LINKS
    part = sub // 2
    me = lax.axis_index("mp")
    z = lax.axis_index("ffn")
    core = lax.rem(me, 2)
    xpos = lax.rem(lax.div(me, 2), 4)
    ypos = lax.div(me, 8)
    sib = 1 - core
    sibling = me + 1 - 2 * core

    bits, peers = [], []
    for pos, stride in ((xpos, 2), (ypos, 8)):
        bits.append(lax.rem(lax.div(pos + 1, 2), 2))
        peers.append(me + stride * (1 - 2 * lax.rem(pos, 2)))
    for pos, stride in ((xpos, 2), (ypos, 8)):
        bits.append(lax.div(pos, 2))
        peers.append(me + stride * (lax.rem(pos + 1 + 2 * lax.rem(pos + 1, 2), 4) - pos))

    def bit(s, stage):
        return bits[(s + stage) % 4]

    def peer(s, stage):
        return peers[(s + stage) % 4]

    def along_z(j):
        return lax.rem(z + j, 4)

    def remote(src, dst, send, recv, mp, ffn):
        return pltpu.make_async_remote_copy(
            src_ref=src, dst_ref=dst, send_sem=send, recv_sem=recv,
            device_id={"mp": mp, "ffn": ffn}, device_id_type=MESH,
        )

    def lanes(start, size):
        return pl.ds(pl.multiple_of(start, 128), size)

    def sublanes(start, size):
        return pl.ds(pl.multiple_of(start, 16), size)

    mine, theirs = lanes(core * depth, depth), lanes(sib * depth, depth)
    my_rows, their_rows = sublanes(core * depth, depth), sublanes(sib * depth, depth)

    pieces = [(0, 0), (1, 0), (0, 1), (1, 1)]
    token_load = pltpu.make_async_copy(tokens, x.at[0, :, mine], load_sem.at[0])
    token_load.start()
    for a, e in pieces:
        cols = pl.ds(a * half + e * quarter, quarter)
        from_cols = lanes(sib * units + a * half + e * quarter, quarter)
        for m, ref in enumerate((gate, up)):
            pltpu.make_async_copy(ref.at[:, from_cols], ws.at[m, :, cols], load_sem.at[1 + e]).start()
    own_loads = []
    for m, ref in enumerate((gate, up)):
        own_loads.append(pltpu.make_async_copy(
            ref.at[:, lanes(core * units, units)], w.at[m, my_rows, :], load_sem.at[3 + m]))
        own_loads[-1].start()
    down_load = pltpu.make_async_copy(
        down.at[sublanes(core * units, units), :], dw.at[:, mine], load_sem.at[5])
    down_load.start()

    def wait_staged(e):
        pltpu.make_async_copy(gate.at[:, pl.ds(0, units)], ws.at[0], load_sem.at[1 + e]).wait()

    barrier = pltpu.get_barrier_semaphore()
    partners = [(sibling, z)] + [(q, z) for q in peers] + [(me, along_z(j)) for j in range(1, 4)]
    for mp, ffn in partners:
        pl.semaphore_signal(barrier, inc=1, device_id={"mp": mp, "ffn": ffn}, device_id_type=MESH)

    def by_rows(count, body):
        def step(i, carry):
            body(lax.div(i, count), lax.rem(i, count) * 16)
            return carry

        lax.fori_loop(0, 2 * count, step, 0)

    def own_part(e):
        wait_staged(e)
        for a in range(2):
            cols = pl.ds(a * half + e * quarter, quarter)
            for m in range(2):
                p[1, 2 * a + e, m] = jnp.dot(x[0, :, mine], ws[m, :, cols], preferred_element_type=F32)
        for s in range(LINKS):

            def body(m, at, s=s):
                rs = sublanes(s * sub + at, 16)
                sx[e, m, rs, :] = coded(p[1, 2 * (1 - bit(s, 0)) + e, m, rs, :])

            by_rows(sub // 16, body)

    with jax.named_scope("z_tload"):
        token_load.wait()
    with jax.named_scope("z_own0"):
        own_part(0)
    with jax.named_scope("z_barrier"):
        pl.semaphore_wait(barrier, len(partners))

    def token_copy(j):
        return remote(x.at[0, :, mine], x.at[4 - j, :, mine], ssem.at[7], tok_sem.at[4 - j], me, along_z(j))

    def relay_copy(j):
        block = x.at[j, :, mine]
        return remote(block, block, ssem.at[8], relay_sem.at[j], sibling, z)

    def weight_copy(i):
        a, e = pieces[i]
        cols = pl.ds(a * half + e * quarter, quarter)
        return remote(ws.at[:, :, cols], w.at[:, my_rows, cols], ssem.at[9], w_sem.at[e], sibling, z)

    def wait_weights(e):
        block = ws.at[:, :, pl.ds(0, half)]
        remote(block, block, ssem.at[9], w_sem.at[e], sibling, z).wait_recv()

    down_copy = remote(
        down.at[sublanes(sib * units, units), :], dw.at[:, mine], ssem.at[10], w_sem.at[2], sibling, z)

    def part_copy(e):
        return remote(sx.at[e], rx.at[e], ssem.at[11], sx_sem.at[e], sibling, z)

    for j in (1, 3, 2):
        token_copy(j).start()
    part_copy(0).start()
    relay_copy(0).start()
    with jax.named_scope("z_own1"):
        own_part(1)
    part_copy(1).start()
    weight_copy(0).start()
    weight_copy(1).start()

    def partial(j, i):
        a, e = pieces[i]
        cols = pl.ds(a * half + e * quarter, quarter)
        for m in range(2):
            p[j, 2 * a + e, m] = jnp.dot(x[j], w[m, :, cols], preferred_element_type=F32)

    def first_copy(j, e, s):
        rs = pl.ds(s * sub, sub)
        return remote(
            s1.at[j, e, :, rs, :], r1.at[j, e, :, rs, :], ssem.at[0], rsem0.at[j, e], peer(s, 0), z)

    def first(j, e):
        for s in range(LINKS):

            def body(m, at, s=s):
                rs = sublanes(s * sub + at, 16)
                s1[j, e, m, rs, :] = coded(p[j, 2 * (1 - bit(s, 0)) + e, m, rs, :])

            by_rows(sub // 16, body)
            first_copy(j, e, s).start()

    def received(block, sem):
        remote(block, block, ssem.at[0], sem, sibling, z).wait_recv()

    with jax.named_scope("z_load"):
        for load in own_loads:
            load.wait()
    with jax.named_scope("z_d0"):
        for i in range(4):
            a, e = pieces[i]
            cols = pl.ds(a * half + e * quarter, quarter)
            for m in range(2):
                p[0, 2 * a + e, m] = jnp.dot(x[0, :, mine], w[m, my_rows, cols], preferred_element_type=F32)
    for e in range(2):
        with jax.named_scope("z_f0%d" % e):
            part_copy(e).wait_recv()
            for s in range(LINKS):

                def body(m, at, s=s, e=e):
                    rs = sublanes(s * sub + at, 16)
                    own = p[0, 2 * (1 - bit(s, 0)) + e, m, rs, :]
                    s1[0, e, m, rs, :] = coded(own + decoded(rx[e, m, rs, :]))

                by_rows(sub // 16, body)
                first_copy(0, e, s).start()
    with jax.named_scope("z_tok"):
        for j in (1, 3):
            token_copy(4 - j).wait_recv()
            relay_copy(j).start()
    weight_copy(2).start()
    with jax.named_scope("z_w0"):
        wait_weights(0)
    with jax.named_scope("z_rel1"):
        relay_copy(1).wait_recv()
    with jax.named_scope("z_f10"):
        partial(1, 0)
        partial(1, 1)
        first(1, 0)
    with jax.named_scope("z_tok2"):
        token_copy(2).wait_recv()
        relay_copy(2).start()
    weight_copy(3).start()
    with jax.named_scope("z_w23"):
        wait_weights(1)
    with jax.named_scope("z_f11"):
        partial(1, 2)
        partial(1, 3)
        first(1, 1)
    for j in (3, 2):
        with jax.named_scope("z_f%d" % j):
            relay_copy(j).wait_recv()
            for e in range(2):
                partial(j, 2 * e)
                partial(j, 2 * e + 1)
                first(j, e)
    down_copy.start()

    with jax.named_scope("z_rest"):
        relay_copy(0).wait_recv()
        for a, e in pieces:
            cols = pl.ds(a * half + e * quarter, quarter)
            for m in range(2):
                p[0, 2 * a + e, m] += jnp.dot(
                    x[0, :, theirs], w[m, their_rows, cols], preferred_element_type=F32)

    def second_copy(j, s):
        rs = pl.ds(s * sub, sub)
        return remote(s2.at[j, :, rs, :], r2.at[j, :, rs, :], ssem.at[1], rsem.at[0, j], peer(s, 1), z)

    def second(j):
        def add(dst, s, e, done):
            def body(m, at):
                rs = sublanes(s * sub + at, 16)
                dst[j, m, rs, :] = done(p[j, 2 * bit(s, 0) + e, m, rs, :] + decoded(r1[j, e, m, rs, :]))

            by_rows(sub // 16, body)

        for e in range(2):
            received(r1.at[j, e], rsem0.at[j, e])
        for s in range(LINKS):
            add(s2, s, 1 - bit(s, 1), coded)
            second_copy(j, s).start()
        for s in range(LINKS):
            add(k2, s, bit(s, 1), lambda v: v)

    def third_copy(j, s):
        rs = pl.ds(s * part, part)
        return remote(s3.at[j, :, rs, :], r3.at[j, :, rs, :], ssem.at[2], rsem.at[1, j], peer(s, 2), z)

    def third(j):
        def add(dst, s, side, done):
            def body(m, at):
                rs = sublanes(s * part + at, 16)
                src = sublanes(s * sub + side * part + at, 16)
                dst[j, m, rs, :] = done(k2[j, m, src, :] + decoded(r2[j, m, src, :]))

            by_rows(part // 16, body)

        received(r2.at[j], rsem.at[0, j])
        for s in range(LINKS):
            add(s3, s, 1 - bit(s, 2), coded)
            third_copy(j, s).start()
        for s in range(LINKS):
            add(k3, s, bit(s, 2), lambda v: v)

    def fourth_copy(j, s):
        rs = pl.ds(s * part, part)
        return remote(s4.at[j, :, rs, :], r4.at[j, :, rs, :], ssem.at[3], rsem.at[2, j], peer(s, 3), z)

    def fourth(j):
        received(r3.at[j], rsem.at[1, j])
        for s in range(LINKS):

            def body(m, at, s=s):
                rs = sublanes(s * part + at, 16)
                v = k3[j, m, rs, :] + decoded(r3[j, m, rs, :])
                k3[j, m, rs, :] = v
                s4[j, m, rs, :] = coded(v)

            by_rows(part // 16, body)
            fourth_copy(j, s).start()

    def gather_copy(step, j, s):
        row, col = s * sub, bit(s, 0) * half
        n_rows, n_cols = sub, half
        if step < 2:
            col, n_cols = col + bit(s, 1) * quarter, quarter
        if step < 1:
            row, n_rows = row + bit(s, 2) * part, part
        block = h.at[j, sublanes(row, n_rows), lanes(col, n_cols)]
        return remote(block, block, ssem.at[4 + step], rsem.at[3 + step, j], peer(s, 2 - step), z)

    def hidden(j):
        received(r4.at[j], rsem.at[2, j])
        for s in range(LINKS):
            row, cols = s * sub + bit(s, 2) * part, lanes(bit(s, 0) * half + bit(s, 1) * quarter, quarter)

            def body(i, carry, s=s, row=row, cols=cols):
                rs = sublanes(s * part + i * 16, 16)
                g = k3[j, 0, rs, :] + decoded(r4[j, 0, rs, :])
                u = k3[j, 1, rs, :] + decoded(r4[j, 1, rs, :])
                value = g / (1.0 + jnp.exp(-g)) * u
                h[j, sublanes(row + i * 16, 16), cols] = value.astype(BF16)
                return carry

            lax.fori_loop(0, part // 16, body, 0)
            gather_copy(0, j, s).start()

    def gathered(step, j):
        size = (part, sub, 2 * sub)[step]
        received(h.at[j, pl.ds(0, size), :], rsem.at[3 + step, j])

    def gather(step, j):
        gathered(step - 1, j)
        for s in range(LINKS):
            gather_copy(step, j, s).start()

    def phase(name, order, run):
        for j in order:
            with jax.named_scope("z_%s%d" % (name, j)):
                run(j)

    phase("second", ORDERS[1], second)
    phase("third", ORDERS[2], third)
    phase("fourth", ORDERS[3], fourth)
    phase("hidden", ORDERS[3], hidden)
    phase("ga", ORDERS[3], lambda j: gather(1, j))
    phase("gb", ORDERS[3], lambda j: gather(2, j))

    down_load.wait()
    down_copy.wait_recv()

    def swap_copy(j):
        return remote(od.at[j], rd.at[j], ssem.at[12], swap_sem.at[j], sibling, z)

    def owner_copy(j):
        return remote(tc.at[j], zr.at[3 - j], ssem.at[13], own_sem.at[4 - j], me, along_z(j))

    def project(j):
        with jax.named_scope("z_gc%d" % j):
            gathered(2, j)
        with jax.named_scope("z_dot%d" % j):
            od[j] = jnp.dot(h[j], dw[:, theirs], preferred_element_type=F32)
            swap_copy(j).start()
            t[j] = jnp.dot(h[j], dw[:, mine], preferred_element_type=F32)

    def to_owner(j):
        with jax.named_scope("z_swap%d" % j):
            swap_copy(j).wait_recv()
        tc[j] = coded(t[j] + rd[j])
        owner_copy(j).start()

    for j in ORDERS[3]:
        project(j)
        if j:
            to_owner(j)

    for i, sent in enumerate((
        s1, s2, s3, s4, h.at[0, pl.ds(0, rows // 2), :], h.at[0], h.at[pl.ds(0, 2)],
        x.at[pl.ds(0, 3), :, mine], x.at[:, :, mine], ws, None, sx, od,
    )):
        if sent is not None:
            remote(sent, sent, ssem.at[i], rsem.at[0, 0], sibling, z).wait_send()
    down_copy.wait_send()
    with jax.named_scope("z_swap0"):
        swap_copy(0).wait_recv()
    with jax.named_scope("z_own"):
        for j in range(1, 4):
            owner_copy(j).wait_recv()
    sent = tc.at[pl.ds(0, 3)]
    remote(sent, sent, ssem.at[13], rsem.at[0, 0], sibling, z).wait_send()
    total = t[0] + rd[0]
    for j in range(3):
        total += decoded(zr[j])
    out[...] = total.astype(out.dtype)


def local(tokens, gate, up, down):
    rows, depth = tokens.shape
    units = gate.shape[1] // 2
    quarter = units // 4
    sem = pltpu.SemaphoreType.DMA
    tall, low = (STREAMS, 2, rows, quarter), (STREAMS, 2, rows // 2, quarter)
    result = (STREAMS, rows, depth)
    return pl.pallas_call(
        kernel,
        out_shape=pltpu.VMEM((rows, depth), BF16),
        in_specs=[pl.BlockSpec(memory_space=pl.ANY)] * 4,
        out_specs=pl.BlockSpec(memory_space=pltpu.VMEM),
        scratch_shapes=[
            pltpu.VMEM((2, 2 * depth, units), BF16),
            pltpu.VMEM((2, depth, units), BF16),
            pltpu.VMEM((units, 2 * depth), BF16),
            pltpu.VMEM((STREAMS, rows, 2 * depth), BF16),
            pltpu.VMEM((STREAMS, 4, 2, rows, quarter), F32),
            *[pltpu.VMEM((STREAMS, 2, 2, rows, quarter), BF16) for _ in range(2)],
            *[pltpu.VMEM(tall, dtype) for dtype in (BF16, BF16, F32)],
            *[pltpu.VMEM(low, dtype) for dtype in (BF16, BF16, F32)],
            *[pltpu.VMEM(low, dtype) for dtype in (BF16, BF16)],
            pltpu.VMEM((STREAMS, rows, units), BF16),
            pltpu.VMEM(result, F32),
            pltpu.VMEM(result, F32),
            pltpu.VMEM(result, F32),
            pltpu.VMEM(result, BF16),
            pltpu.VMEM((3, rows, depth), BF16),
            *[pltpu.VMEM((2, 2, rows, quarter), BF16) for _ in range(2)],
            sem((14,)),
            sem((STREAMS, 2)),
            sem((6, STREAMS)),
            sem((6,)),
            sem((STREAMS,)),
            sem((STREAMS,)),
            sem((3,)),
            sem((2,)),
            sem((STREAMS,)),
            sem((STREAMS,)),
        ],
        compiler_params=pltpu.CompilerParams(
            collective_id=0, has_side_effects=True, vmem_limit_bytes=60 * 2**20
        ),
    )(tokens, gate, up, down)


def solution(mesh):
    placed = (P("ffn", "mp"), P("mp", "ffn"), P("mp", "ffn"), P("ffn", "mp"))
    return jax.shard_map(
        local, mesh=mesh, in_specs=placed, out_specs=P("ffn", "mp"), check_vma=False
    )
```

```python
import functools
import itertools

import jax
import jax.numpy as jnp
from jax import lax
from jax.experimental import pallas as pl
from jax.experimental.pallas import tpu as pltpu
from jax.sharding import PartitionSpec as P

MESH = pl.DeviceIdType.MESH
STREAMS = 4
LINKS = 4
WAVE = (
    (1, 1), (1, 3), (1, 2), (2, 1), (2, 3), (1, 0), (2, 2), (3, 1),
    (3, 3), (2, 0), (3, 2), (4, 1), (4, 3), (3, 0), (4, 2), (5, 1),
    (5, 3), (4, 0), (5, 2), (6, 1), (6, 2), (5, 0), (6, 3), (7, 1),
    (8, 1), (7, 2), (6, 0), (8, 2), (7, 3), (8, 3), (7, 0),
)
F32 = jnp.float32
BF16 = jnp.bfloat16

PROJECTED = min(i for i, (step, _) in enumerate(WAVE) if step == 7)


def coded(v):
    return (v * jnp.abs(v)).astype(BF16)


def decoded(c):
    u = c.astype(F32)
    return u * lax.rsqrt(jnp.maximum(jnp.abs(u), 1e-37))


def kernel(
    tokens, gate, up, down, out,
    w, ws, dw, x, p, s1, r1, s2, r2, k2, s3, r3, k3, s4, r4, h, od, rd, t, tc, zr,
    sx, rx, ssem, rsem0, rsem, load_sem, tok_sem, relay_sem, w_sem, sx_sem, swap_sem, own_sem,
):
    rows, depth = tokens.shape
    units = w.shape[2]
    half, quarter = units // 2, units // 4
    sub = rows // LINKS
    part = sub // 2
    me = lax.axis_index("mp")
    z = lax.axis_index("ffn")
    core = lax.rem(me, 2)
    xpos = lax.rem(lax.div(me, 2), 4)
    ypos = lax.div(me, 8)
    sib = 1 - core
    sibling = me + 1 - 2 * core

    bits, peers = [], []
    for pos, stride in ((xpos, 2), (ypos, 8)):
        bits.append(lax.rem(lax.div(pos + 1, 2), 2))
        peers.append(me + stride * (1 - 2 * lax.rem(pos, 2)))
    for pos, stride in ((xpos, 2), (ypos, 8)):
        bits.append(lax.div(pos, 2))
        peers.append(me + stride * (lax.rem(pos + 1 + 2 * lax.rem(pos + 1, 2), 4) - pos))

    def bit(s, stage):
        return bits[(s + stage) % 4]

    def peer(s, stage):
        return peers[(s + stage) % 4]

    def along_z(j):
        return lax.rem(z + j, 4)

    def remote(src, dst, send, recv, mp, ffn):
        return pltpu.make_async_remote_copy(
            src_ref=src, dst_ref=dst, send_sem=send, recv_sem=recv,
            device_id={"mp": mp, "ffn": ffn}, device_id_type=MESH,
        )

    def lanes(start, size):
        return pl.ds(pl.multiple_of(start, 128), size)

    def sublanes(start, size):
        return pl.ds(pl.multiple_of(start, 16), size)

    mine, theirs = lanes(core * depth, depth), lanes(sib * depth, depth)
    my_rows, their_rows = sublanes(core * depth, depth), sublanes(sib * depth, depth)

    barrier = pltpu.get_barrier_semaphore()
    partners = [(sibling, z)] + [(q, z) for q in peers] + [(me, along_z(j)) for j in range(1, 4)]
    for mp, ffn in partners:
        pl.semaphore_signal(barrier, inc=1, device_id={"mp": mp, "ffn": ffn}, device_id_type=MESH)

    pieces = [(0, 0), (1, 0), (0, 1), (1, 1)]
    token_load = pltpu.make_async_copy(tokens, x.at[0, :, mine], load_sem.at[8])
    token_load.start()
    for e, own, m in itertools.product(range(2), repeat=3):
        ref = (gate, up)[m]
        for a in range(2):
            at = a * half + e * quarter
            cols, from_cols = pl.ds(at, quarter), lanes((core if own else sib) * units + at, quarter)
            dst = w.at[m, my_rows, cols] if own else ws.at[m, :, cols]
            pltpu.make_async_copy(ref.at[:, from_cols], dst, load_sem.at[4 * e + 2 * own + m]).start()
    down_load = pltpu.make_async_copy(
        down.at[sublanes(core * units, units), :], dw.at[:, mine], load_sem.at[9])
    down_load.start()

    def wait_loaded(e, own, m):
        pltpu.make_async_copy(
            gate.at[:, pl.ds(0, half)], ws.at[0, :, pl.ds(0, half)], load_sem.at[4 * e + 2 * own + m]).wait()

    def own_part(e, m):
        wait_loaded(e, 0, m)
        for a in range(2):
            cols = pl.ds(a * half + e * quarter, quarter)
            p[1, 2 * a + e, m] = jnp.dot(x[0, :, mine], ws[m, :, cols], preferred_element_type=F32)
        for s in range(LINKS):
            rs = pl.ds(s * sub, sub)
            sx[e, m, rs, :] = coded(p[1, 2 * (1 - bit(s, 0)) + e, m, rs, :])

    with jax.named_scope("z_tload"):
        token_load.wait()
    with jax.named_scope("z_own0"):
        own_part(0, 0)
    with jax.named_scope("z_barrier"):
        pl.semaphore_wait(barrier, len(partners))

    def token_copy(j):
        return remote(x.at[0, :, mine], x.at[4 - j, :, mine], ssem.at[7], tok_sem.at[4 - j], me, along_z(j))

    def relay_copy(j):
        block = x.at[j, :, mine]
        return remote(block, block, ssem.at[8], relay_sem.at[j], sibling, z)

    def weight_copy(i):
        a, e = pieces[i]
        cols = pl.ds(a * half + e * quarter, quarter)
        return remote(ws.at[:, :, cols], w.at[:, my_rows, cols], ssem.at[9], w_sem.at[e], sibling, z)

    def wait_weights(e):
        block = ws.at[:, :, pl.ds(0, half)]
        remote(block, block, ssem.at[9], w_sem.at[e], sibling, z).wait_recv()

    down_copy = remote(
        down.at[sublanes(sib * units, units), :], dw.at[:, mine], ssem.at[10], w_sem.at[2], sibling, z)

    def part_copy(e, m):
        return remote(sx.at[e, m], rx.at[e, m], ssem.at[11], sx_sem.at[2 * e + m], sibling, z)

    def own_rows(e, m):
        wait_loaded(e, 1, m)
        for a in range(2):
            cols = pl.ds(a * half + e * quarter, quarter)
            p[0, 2 * a + e, m] = jnp.dot(x[0, :, mine], w[m, my_rows, cols], preferred_element_type=F32)

    part_copy(0, 0).start()
    for j in (1, 3, 2):
        token_copy(j).start()
    with jax.named_scope("z_own01"):
        own_part(0, 1)
        part_copy(0, 1).start()
    relay_copy(0).start()
    weight_copy(0).start()
    with jax.named_scope("z_d0"):
        for m in range(2):
            own_rows(0, m)

    def partial(j, i):
        a, e = pieces[i]
        cols = pl.ds(a * half + e * quarter, quarter)
        for m in range(2):
            p[j, 2 * a + e, m] = jnp.dot(x[j], w[m, :, cols], preferred_element_type=F32)

    def first_copy(j, e, s):
        rs = pl.ds(s * sub, sub)
        return remote(
            s1.at[j, e, :, rs, :], r1.at[j, e, :, rs, :], ssem.at[0], rsem0.at[j, e], peer(s, 0), z)

    def half_copy(e, s, m):
        rs = pl.ds(s * sub, sub)
        return remote(
            s1.at[0, e, m, rs, :], r1.at[0, e, m, rs, :], ssem.at[0], rsem0.at[0, e], peer(s, 0), z)

    def first(j, e):
        for s in range(LINKS):

            rs = pl.ds(s * sub, sub)
            for m in range(2):
                s1[j, e, m, rs, :] = coded(p[j, 2 * (1 - bit(s, 0)) + e, m, rs, :])
            first_copy(j, e, s).start()

    def received(block, sem):
        remote(block, block, ssem.at[0], sem, sibling, z).wait_recv()

    for e in range(2):
        with jax.named_scope("z_f0%d" % e):
            for m in range(2):
                part_copy(e, m).wait_recv()
                for s in range(LINKS):
                    rs = pl.ds(s * sub, sub)
                    own = p[0, 2 * (1 - bit(s, 0)) + e, m, rs, :]
                    s1[0, e, m, rs, :] = coded(own + decoded(rx[e, m, rs, :]))
                    half_copy(e, s, m).start()
        if e == 0:
            with jax.named_scope("z_own1"):
                for m in range(2):
                    own_part(1, m)
                    part_copy(1, m).start()
                weight_copy(1).start()
                for m in range(2):
                    own_rows(1, m)
    with jax.named_scope("z_tok"):
        for j in (1, 3):
            token_copy(4 - j).wait_recv()
            relay_copy(j).start()
    weight_copy(2).start()
    weight_copy(3).start()
    with jax.named_scope("z_w0"):
        wait_weights(0)
    with jax.named_scope("z_rel1"):
        relay_copy(1).wait_recv()
    with jax.named_scope("z_f10"):
        partial(1, 0)
        partial(1, 1)
        first(1, 0)
    with jax.named_scope("z_tok2"):
        token_copy(2).wait_recv()
        relay_copy(2).start()
    with jax.named_scope("z_w23"):
        wait_weights(1)
    down_copy.start()
    with jax.named_scope("z_f11"):
        partial(1, 2)
        partial(1, 3)
        first(1, 1)
    for j in (3, 2):
        with jax.named_scope("z_f%d" % j):
            relay_copy(j).wait_recv()
            for e in range(2):
                partial(j, 2 * e)
                partial(j, 2 * e + 1)
                first(j, e)

    with jax.named_scope("z_rest"):
        relay_copy(0).wait_recv()
        for a, e in pieces:
            cols = pl.ds(a * half + e * quarter, quarter)
            for m in range(2):
                p[0, 2 * a + e, m] += jnp.dot(
                    x[0, :, theirs], w[m, their_rows, cols], preferred_element_type=F32)

    def second_copy(j, s):
        rs = pl.ds(s * sub, sub)
        return remote(s2.at[j, :, rs, :], r2.at[j, :, rs, :], ssem.at[1], rsem.at[0, j], peer(s, 1), z)

    def second(j):
        def add(dst, s, e, done):
            rs = pl.ds(s * sub, sub)
            for m in range(2):
                dst[j, m, rs, :] = done(p[j, 2 * bit(s, 0) + e, m, rs, :] + decoded(r1[j, e, m, rs, :]))

        for e in range(2):
            received(r1.at[j, e], rsem0.at[j, e])
        for s in range(LINKS):
            add(s2, s, 1 - bit(s, 1), coded)
            second_copy(j, s).start()
        for s in range(LINKS):
            add(k2, s, bit(s, 1), lambda v: v)

    def third_copy(j, s):
        rs = pl.ds(s * part, part)
        return remote(s3.at[j, :, rs, :], r3.at[j, :, rs, :], ssem.at[2], rsem.at[1, j], peer(s, 2), z)

    def third(j):
        def add(dst, s, side, done):
            rs, src = pl.ds(s * part, part), sublanes(s * sub + side * part, part)
            for m in range(2):
                dst[j, m, rs, :] = done(k2[j, m, src, :] + decoded(r2[j, m, src, :]))

        received(r2.at[j], rsem.at[0, j])
        for s in range(LINKS):
            add(s3, s, 1 - bit(s, 2), coded)
            third_copy(j, s).start()
        for s in range(LINKS):
            add(k3, s, bit(s, 2), lambda v: v)

    def fourth_copy(j, s):
        rs = pl.ds(s * part, part)
        return remote(s4.at[j, :, rs, :], r4.at[j, :, rs, :], ssem.at[3], rsem.at[2, j], peer(s, 3), z)

    def fourth(j):
        received(r3.at[j], rsem.at[1, j])
        for s in range(LINKS):
            rs = pl.ds(s * part, part)
            for m in range(2):
                v = k3[j, m, rs, :] + decoded(r3[j, m, rs, :])
                k3[j, m, rs, :] = v
                s4[j, m, rs, :] = coded(v)
            fourth_copy(j, s).start()

    def gather_copy(step, j, s):
        row, col = s * sub, bit(s, 0) * half
        n_rows, n_cols = sub, half
        if step < 2:
            col, n_cols = col + bit(s, 1) * quarter, quarter
        if step < 1:
            row, n_rows = row + bit(s, 2) * part, part
        block = h.at[j, sublanes(row, n_rows), lanes(col, n_cols)]
        return remote(block, block, ssem.at[4 + step], rsem.at[3 + step, j], peer(s, 2 - step), z)

    def hidden(j):
        received(r4.at[j], rsem.at[2, j])
        for s in range(LINKS):
            row, cols = s * sub + bit(s, 2) * part, lanes(bit(s, 0) * half + bit(s, 1) * quarter, quarter)
            rs = pl.ds(s * part, part)
            g = k3[j, 0, rs, :] + decoded(r4[j, 0, rs, :])
            u = k3[j, 1, rs, :] + decoded(r4[j, 1, rs, :])
            value = g / (1.0 + jnp.exp(-g)) * u
            h[j, sublanes(row, part), cols] = value.astype(BF16)
            gather_copy(0, j, s).start()

    def gathered(step, j):
        size = (part, sub, 2 * sub)[step]
        received(h.at[j, pl.ds(0, size), :], rsem.at[3 + step, j])

    def gather(step, j):
        gathered(step - 1, j)
        for s in range(LINKS):
            gather_copy(step, j, s).start()


    def swap_copy(j):
        return remote(od.at[j], rd.at[j], ssem.at[12], swap_sem.at[j], sibling, z)

    def owner_copy(j):
        return remote(tc.at[j], zr.at[3 - j], ssem.at[13], own_sem.at[4 - j], me, along_z(j))

    def project(j):
        with jax.named_scope("z_gc%d" % j):
            gathered(2, j)
        with jax.named_scope("z_dot%d" % j):
            od[j] = jnp.dot(h[j], dw[:, theirs], preferred_element_type=F32)
            swap_copy(j).start()
            t[j] = jnp.dot(h[j], dw[:, mine], preferred_element_type=F32)

    def to_owner(j):
        with jax.named_scope("z_swap%d" % j):
            swap_copy(j).wait_recv()
        tc[j] = coded(t[j] + rd[j])
        owner_copy(j).start()

    steps = (
        second, third, fourth, hidden, functools.partial(gather, 1), functools.partial(gather, 2), project, to_owner,
    )
    for i, (step, j) in enumerate(WAVE):
        if i == PROJECTED:
            down_load.wait()
            down_copy.wait_recv()
        with jax.named_scope("z_st%d_%d" % (step, j)):
            steps[step - 1](j)

    for i, sent in enumerate((
        s1, s2, s3, s4, h.at[0, pl.ds(0, rows // 2), :], h.at[0], h.at[pl.ds(0, 2)],
        x.at[pl.ds(0, 3), :, mine], x.at[:, :, mine], ws, None, sx, od,
    )):
        if sent is not None:
            remote(sent, sent, ssem.at[i], rsem.at[0, 0], sibling, z).wait_send()
    down_copy.wait_send()
    with jax.named_scope("z_swap0"):
        swap_copy(0).wait_recv()
    with jax.named_scope("z_own"):
        for j in range(1, 4):
            owner_copy(j).wait_recv()
    sent = tc.at[pl.ds(0, 3)]
    remote(sent, sent, ssem.at[13], rsem.at[0, 0], sibling, z).wait_send()
    total = t[0] + rd[0]
    for j in range(3):
        total += decoded(zr[j])
    out[...] = total.astype(out.dtype)


def local(tokens, gate, up, down):
    rows, depth = tokens.shape
    units = gate.shape[1] // 2
    quarter = units // 4
    sem = pltpu.SemaphoreType.DMA
    tall, low = (STREAMS, 2, rows, quarter), (STREAMS, 2, rows // 2, quarter)
    result = (STREAMS, rows, depth)
    return pl.pallas_call(
        kernel,
        out_shape=pltpu.VMEM((rows, depth), BF16),
        in_specs=[pl.BlockSpec(memory_space=pl.ANY)] * 4,
        out_specs=pl.BlockSpec(memory_space=pltpu.VMEM),
        scratch_shapes=[
            pltpu.VMEM((2, 2 * depth, units), BF16),
            pltpu.VMEM((2, depth, units), BF16),
            pltpu.VMEM((units, 2 * depth), BF16),
            pltpu.VMEM((STREAMS, rows, 2 * depth), BF16),
            pltpu.VMEM((STREAMS, 4, 2, rows, quarter), F32),
            *[pltpu.VMEM((STREAMS, 2, 2, rows, quarter), BF16) for _ in range(2)],
            *[pltpu.VMEM(tall, dtype) for dtype in (BF16, BF16, F32)],
            *[pltpu.VMEM(low, dtype) for dtype in (BF16, BF16, F32)],
            *[pltpu.VMEM(low, dtype) for dtype in (BF16, BF16)],
            pltpu.VMEM((STREAMS, rows, units), BF16),
            pltpu.VMEM(result, F32),
            pltpu.VMEM(result, F32),
            pltpu.VMEM(result, F32),
            pltpu.VMEM(result, BF16),
            pltpu.VMEM((3, rows, depth), BF16),
            *[pltpu.VMEM((2, 2, rows, quarter), BF16) for _ in range(2)],
            sem((14,)),
            sem((STREAMS, 2)),
            sem((6, STREAMS)),
            sem((10,)),
            sem((STREAMS,)),
            sem((STREAMS,)),
            sem((3,)),
            sem((4,)),
            sem((STREAMS,)),
            sem((STREAMS,)),
        ],
        compiler_params=pltpu.CompilerParams(
            collective_id=0, has_side_effects=True, vmem_limit_bytes=60 * 2**20
        ),
    )(tokens, gate, up, down)


def solution(mesh):
    placed = (P("ffn", "mp"), P("mp", "ffn"), P("mp", "ffn"), P("ffn", "mp"))
    return jax.shard_map(
        local, mesh=mesh, in_specs=placed, out_specs=P("ffn", "mp"), check_vma=False
    )
```

```python
import functools
import itertools

import jax
import jax.numpy as jnp
from jax import lax
from jax.experimental import pallas as pl
from jax.experimental.pallas import tpu as pltpu
from jax.sharding import PartitionSpec as P

MESH = pl.DeviceIdType.MESH
STREAMS = 4
LINKS = 4
WAVE = (
    (1, 1), (1, 3), (1, 2), (2, 1), (2, 3), (1, 0), (2, 2), (3, 1),
    (3, 3), (2, 0), (3, 2), (4, 1), (4, 3), (3, 0), (4, 2), (5, 1),
    (5, 3), (4, 0), (5, 2), (6, 1), (6, 2), (5, 0), (6, 3), (7, 1),
    (8, 1), (7, 2), (6, 0), (8, 2), (7, 3), (8, 3), (7, 0),
)
F32 = jnp.float32
BF16 = jnp.bfloat16

PROJECTED = min(i for i, (step, _) in enumerate(WAVE) if step == 7)


def coded(v):
    return (v * jnp.abs(v)).astype(BF16)


def decoded(c):
    u = c.astype(F32)
    return u * lax.rsqrt(jnp.maximum(jnp.abs(u), 1e-37))


def kernel(
    tokens, gate, up, down, out,
    w, ws, dw, x, p, s1, r1, s2, r2, k2, s3, r3, k3, s4, r4, h, od, rd, t, tc, zr,
    sx, rx, ssem, rsem0, rsem, load_sem, tok_sem, relay_sem, w_sem, sx_sem, swap_sem, own_sem,
):
    rows, depth = tokens.shape
    units = w.shape[2]
    half, quarter = units // 2, units // 4
    sub = rows // LINKS
    part = sub // 2
    me = lax.axis_index("mp")
    z = lax.axis_index("ffn")
    core = lax.rem(me, 2)
    xpos = lax.rem(lax.div(me, 2), 4)
    ypos = lax.div(me, 8)
    sib = 1 - core
    sibling = me + 1 - 2 * core

    bits, peers = [], []
    for pos, stride in ((xpos, 2), (ypos, 8)):
        bits.append(lax.rem(lax.div(pos + 1, 2), 2))
        peers.append(me + stride * (1 - 2 * lax.rem(pos, 2)))
    for pos, stride in ((xpos, 2), (ypos, 8)):
        bits.append(lax.div(pos, 2))
        peers.append(me + stride * (lax.rem(pos + 1 + 2 * lax.rem(pos + 1, 2), 4) - pos))

    def bit(s, stage):
        return bits[(s + stage) % 4]

    def peer(s, stage):
        return peers[(s + stage) % 4]

    def along_z(j):
        return lax.rem(z + j, 4)

    def remote(src, dst, send, recv, mp, ffn):
        return pltpu.make_async_remote_copy(
            src_ref=src, dst_ref=dst, send_sem=send, recv_sem=recv,
            device_id={"mp": mp, "ffn": ffn}, device_id_type=MESH,
        )

    def lanes(start, size):
        return pl.ds(pl.multiple_of(start, 128), size)

    def sublanes(start, size):
        return pl.ds(pl.multiple_of(start, 16), size)

    mine, theirs = lanes(core * depth, depth), lanes(sib * depth, depth)
    my_rows, their_rows = sublanes(core * depth, depth), sublanes(sib * depth, depth)

    barrier = pltpu.get_barrier_semaphore()
    partners = [(sibling, z)] + [(q, z) for q in peers] + [(me, along_z(j)) for j in range(1, 4)]
    for mp, ffn in partners:
        pl.semaphore_signal(barrier, inc=1, device_id={"mp": mp, "ffn": ffn}, device_id_type=MESH)

    pieces = [(0, 0), (1, 0), (0, 1), (1, 1)]
    token_load = pltpu.make_async_copy(tokens, x.at[0, :, mine], load_sem.at[8])
    token_load.start()
    for e, own, m in itertools.product(range(2), repeat=3):
        ref = (gate, up)[m]
        for a in range(2):
            at = a * half + e * quarter
            cols, from_cols = pl.ds(at, quarter), lanes((core if own else sib) * units + at, quarter)
            dst = w.at[m, my_rows, cols] if own else ws.at[m, :, cols]
            pltpu.make_async_copy(ref.at[:, from_cols], dst, load_sem.at[4 * e + 2 * own + m]).start()
    down_load = pltpu.make_async_copy(
        down.at[sublanes(core * units, units), :], dw.at[:, mine], load_sem.at[9])
    down_load.start()

    def wait_loaded(e, own, m):
        pltpu.make_async_copy(
            gate.at[:, pl.ds(0, half)], ws.at[0, :, pl.ds(0, half)], load_sem.at[4 * e + 2 * own + m]).wait()

    def own_part(e, m):
        wait_loaded(e, 0, m)
        for a in range(2):
            cols = pl.ds(a * half + e * quarter, quarter)
            p[1, 2 * a + e, m] = jnp.dot(x[0, :, mine], ws[m, :, cols], preferred_element_type=F32)
        for s in range(LINKS):
            rs = pl.ds(s * sub, sub)
            sx[e, m, rs, :] = coded(p[1, 2 * (1 - bit(s, 0)) + e, m, rs, :])

    with jax.named_scope("z_tload"):
        token_load.wait()
    with jax.named_scope("z_own0"):
        own_part(0, 0)
    with jax.named_scope("z_barrier"):
        pl.semaphore_wait(barrier, len(partners))

    def token_copy(j):
        return remote(x.at[0, :, mine], x.at[4 - j, :, mine], ssem.at[7], tok_sem.at[3 - j], me, along_z(j))

    def relay_copy(j):
        block = x.at[j, :, mine]
        return remote(block, block, ssem.at[8], relay_sem.at[j], sibling, z)

    def weight_copy(i):
        a, e = pieces[i]
        cols = pl.ds(a * half + e * quarter, quarter)
        return remote(ws.at[:, :, cols], w.at[:, my_rows, cols], ssem.at[9], w_sem.at[e], sibling, z)

    def wait_weights(e):
        block = ws.at[:, :, pl.ds(0, half)]
        remote(block, block, ssem.at[9], w_sem.at[e], sibling, z).wait_recv()

    down_copy = remote(
        down.at[sublanes(sib * units, units), :], dw.at[:, mine], ssem.at[10], w_sem.at[2], sibling, z)

    def part_copy(e, m):
        return remote(sx.at[e, m], rx.at[e, m], ssem.at[11], sx_sem.at[2 * e + m], sibling, z)

    def own_rows(e, m):
        wait_loaded(e, 1, m)
        for a in range(2):
            cols = pl.ds(a * half + e * quarter, quarter)
            p[0, 2 * a + e, m] = jnp.dot(x[0, :, mine], w[m, my_rows, cols], preferred_element_type=F32)

    part_copy(0, 0).start()
    for j in (1, 3, 2):
        token_copy(j).start()
    with jax.named_scope("z_own01"):
        own_part(0, 1)
        part_copy(0, 1).start()
    relay_copy(0).start()
    weight_copy(0).start()
    with jax.named_scope("z_d0"):
        for m in range(2):
            own_rows(0, m)

    def partial(j, i):
        a, e = pieces[i]
        cols = pl.ds(a * half + e * quarter, quarter)
        for m in range(2):
            p[j, 2 * a + e, m] = jnp.dot(x[j], w[m, :, cols], preferred_element_type=F32)

    def first_copy(j, e, s):
        rs = pl.ds(s * sub, sub)
        return remote(
            s1.at[j, e, :, rs, :], r1.at[j, e, :, rs, :], ssem.at[0], rsem0.at[j], peer(s, 0), z)

    def half_copy(e, s, m):
        rs = pl.ds(s * sub, sub)
        return remote(
            s1.at[0, e, m, rs, :], r1.at[0, e, m, rs, :], ssem.at[0], rsem0.at[0], peer(s, 0), z)

    def first(j, e):
        for s in range(LINKS):

            rs = pl.ds(s * sub, sub)
            for m in range(2):
                s1[j, e, m, rs, :] = coded(p[j, 2 * (1 - bit(s, 0)) + e, m, rs, :])
            first_copy(j, e, s).start()

    def received(block, sem):
        remote(block, block, ssem.at[0], sem, sibling, z).wait_recv()

    for e in range(2):
        with jax.named_scope("z_f0%d" % e):
            for m in range(2):
                part_copy(e, m).wait_recv()
                for s in range(LINKS):
                    rs = pl.ds(s * sub, sub)
                    own = p[0, 2 * (1 - bit(s, 0)) + e, m, rs, :]
                    s1[0, e, m, rs, :] = coded(own + decoded(rx[e, m, rs, :]))
                    half_copy(e, s, m).start()
        if e == 0:
            with jax.named_scope("z_own1"):
                for m in range(2):
                    own_part(1, m)
                    part_copy(1, m).start()
                weight_copy(1).start()
                for m in range(2):
                    own_rows(1, m)
    with jax.named_scope("z_tok"):
        for j in (1, 3):
            token_copy(4 - j).wait_recv()
            relay_copy(j).start()
    weight_copy(2).start()
    weight_copy(3).start()
    with jax.named_scope("z_w0"):
        wait_weights(0)
    with jax.named_scope("z_rel1"):
        relay_copy(1).wait_recv()
    with jax.named_scope("z_f10"):
        partial(1, 0)
        partial(1, 1)
        first(1, 0)
    with jax.named_scope("z_tok2"):
        token_copy(2).wait_recv()
        relay_copy(2).start()
    with jax.named_scope("z_w23"):
        wait_weights(1)
    down_copy.start()
    with jax.named_scope("z_f11"):
        partial(1, 2)
        partial(1, 3)
        first(1, 1)
    for j in (3, 2):
        with jax.named_scope("z_f%d" % j):
            relay_copy(j).wait_recv()
            for e in range(2):
                partial(j, 2 * e)
                partial(j, 2 * e + 1)
                first(j, e)

    with jax.named_scope("z_rest"):
        relay_copy(0).wait_recv()
        for a, e in pieces:
            cols = pl.ds(a * half + e * quarter, quarter)
            for m in range(2):
                p[0, 2 * a + e, m] += jnp.dot(
                    x[0, :, theirs], w[m, their_rows, cols], preferred_element_type=F32)

    def second_copy(j, s):
        rs = pl.ds(s * sub, sub)
        return remote(s2.at[j, :, rs, :], r2.at[j, :, rs, :], ssem.at[1], rsem.at[0, j], peer(s, 1), z)

    def second(j):
        def add(dst, s, e, done):
            rs = pl.ds(s * sub, sub)
            for m in range(2):
                dst[j, m, rs, :] = done(p[j, 2 * bit(s, 0) + e, m, rs, :] + decoded(r1[j, e, m, rs, :]))

        received(r1.at[j], rsem0.at[j])
        for s in range(LINKS):
            add(s2, s, 1 - bit(s, 1), coded)
            second_copy(j, s).start()
        for s in range(LINKS):
            add(k2, s, bit(s, 1), lambda v: v)

    def third_copy(j, s):
        rs = pl.ds(s * part, part)
        return remote(s3.at[j, :, rs, :], r3.at[j, :, rs, :], ssem.at[2], rsem.at[1, j], peer(s, 2), z)

    def third(j):
        def add(dst, s, side, done):
            rs, src = pl.ds(s * part, part), sublanes(s * sub + side * part, part)
            for m in range(2):
                dst[j, m, rs, :] = done(k2[j, m, src, :] + decoded(r2[j, m, src, :]))

        received(r2.at[j], rsem.at[0, j])
        for s in range(LINKS):
            add(s3, s, 1 - bit(s, 2), coded)
            third_copy(j, s).start()
        for s in range(LINKS):
            add(k3, s, bit(s, 2), lambda v: v)

    def fourth_copy(j, s):
        rs = pl.ds(s * part, part)
        return remote(s4.at[j, :, rs, :], r4.at[j, :, rs, :], ssem.at[3], rsem.at[2, j], peer(s, 3), z)

    def fourth(j):
        received(r3.at[j], rsem.at[1, j])
        for s in range(LINKS):
            rs = pl.ds(s * part, part)
            for m in range(2):
                v = k3[j, m, rs, :] + decoded(r3[j, m, rs, :])
                k3[j, m, rs, :] = v
                s4[j, m, rs, :] = coded(v)
            fourth_copy(j, s).start()

    def gather_copy(step, j, s):
        row, col = s * sub, bit(s, 0) * half
        n_rows, n_cols = sub, half
        if step < 2:
            col, n_cols = col + bit(s, 1) * quarter, quarter
        if step < 1:
            row, n_rows = row + bit(s, 2) * part, part
        block = h.at[j, sublanes(row, n_rows), lanes(col, n_cols)]
        return remote(block, block, ssem.at[4 + step], rsem.at[3 + step, j], peer(s, 2 - step), z)

    def hidden(j):
        received(r4.at[j], rsem.at[2, j])
        for s in range(LINKS):
            row, cols = s * sub + bit(s, 2) * part, lanes(bit(s, 0) * half + bit(s, 1) * quarter, quarter)
            rs = pl.ds(s * part, part)
            g = k3[j, 0, rs, :] + decoded(r4[j, 0, rs, :])
            u = k3[j, 1, rs, :] + decoded(r4[j, 1, rs, :])
            value = g / (1.0 + jnp.exp(-g)) * u
            h[j, sublanes(row, part), cols] = value.astype(BF16)
            gather_copy(0, j, s).start()

    def gathered(step, j):
        size = (part, sub, 2 * sub)[step]
        received(h.at[j, pl.ds(0, size), :], rsem.at[3 + step, j])

    def gather(step, j):
        gathered(step - 1, j)
        for s in range(LINKS):
            gather_copy(step, j, s).start()


    def swap_copy(j):
        return remote(od.at[j], rd.at[j], ssem.at[12], swap_sem.at[j], sibling, z)

    def owner_copy(j):
        return remote(tc.at[j], zr.at[3 - j], ssem.at[13], own_sem.at[3 - j], me, along_z(j))

    def project(j):
        with jax.named_scope("z_gc%d" % j):
            gathered(2, j)
        with jax.named_scope("z_dot%d" % j):
            od[j] = jnp.dot(h[j], dw[:, theirs], preferred_element_type=F32)
            swap_copy(j).start()
            t[j] = jnp.dot(h[j], dw[:, mine], preferred_element_type=F32)

    def to_owner(j):
        with jax.named_scope("z_swap%d" % j):
            swap_copy(j).wait_recv()
        tc[j] = coded(t[j] + rd[j])
        owner_copy(j).start()

    steps = (
        second, third, fourth, hidden, functools.partial(gather, 1), functools.partial(gather, 2), project, to_owner,
    )
    for i, (step, j) in enumerate(WAVE):
        if i == PROJECTED:
            down_load.wait()
            down_copy.wait_recv()
        with jax.named_scope("z_st%d_%d" % (step, j)):
            steps[step - 1](j)

    for i, sent in enumerate((
        s1, s2, s3, s4, h.at[0, pl.ds(0, rows // 2), :], h.at[0], h.at[pl.ds(0, 2)],
        x.at[pl.ds(0, 3), :, mine], x.at[:, :, mine], ws, None, sx, od,
    )):
        if sent is not None:
            remote(sent, sent, ssem.at[i], rsem.at[0, 0], sibling, z).wait_send()
    down_copy.wait_send()
    with jax.named_scope("z_swap0"):
        swap_copy(0).wait_recv()
    with jax.named_scope("z_own"):
        for j in range(1, 4):
            owner_copy(j).wait_recv()
    sent = tc.at[pl.ds(0, 3)]
    remote(sent, sent, ssem.at[13], rsem.at[0, 0], sibling, z).wait_send()
    total = t[0] + rd[0]
    for j in range(3):
        total += decoded(zr[j])
    out[...] = total.astype(out.dtype)


def local(tokens, gate, up, down):
    rows, depth = tokens.shape
    units = gate.shape[1] // 2
    quarter = units // 4
    sem = pltpu.SemaphoreType.DMA
    tall, low = (STREAMS, 2, rows, quarter), (STREAMS, 2, rows // 2, quarter)
    result = (STREAMS, rows, depth)
    return pl.pallas_call(
        kernel,
        out_shape=pltpu.VMEM((rows, depth), BF16),
        in_specs=[pl.BlockSpec(memory_space=pl.ANY)] * 4,
        out_specs=pl.BlockSpec(memory_space=pltpu.VMEM),
        scratch_shapes=[
            pltpu.VMEM((2, 2 * depth, units), BF16),
            pltpu.VMEM((2, depth, units), BF16),
            pltpu.VMEM((units, 2 * depth), BF16),
            pltpu.VMEM((STREAMS, rows, 2 * depth), BF16),
            pltpu.VMEM((STREAMS, 4, 2, rows, quarter), F32),
            *[pltpu.VMEM((STREAMS, 2, 2, rows, quarter), BF16) for _ in range(2)],
            *[pltpu.VMEM(tall, dtype) for dtype in (BF16, BF16, F32)],
            *[pltpu.VMEM(low, dtype) for dtype in (BF16, BF16, F32)],
            *[pltpu.VMEM(low, dtype) for dtype in (BF16, BF16)],
            pltpu.VMEM((STREAMS, rows, units), BF16),
            pltpu.VMEM(result, F32),
            pltpu.VMEM(result, F32),
            pltpu.VMEM(result, F32),
            pltpu.VMEM(result, BF16),
            pltpu.VMEM((3, rows, depth), BF16),
            *[pltpu.VMEM((2, 2, rows, quarter), BF16) for _ in range(2)],
            sem((14,)),
            sem((STREAMS,)),
            sem((6, STREAMS)),
            sem((10,)),
            sem((3,)),
            sem((STREAMS,)),
            sem((3,)),
            sem((4,)),
            sem((STREAMS,)),
            sem((3,)),
        ],
        compiler_params=pltpu.CompilerParams(
            collective_id=0, has_side_effects=True, vmem_limit_bytes=60 * 2**20
        ),
    )(tokens, gate, up, down)


def solution(mesh):
    placed = (P("ffn", "mp"), P("mp", "ffn"), P("mp", "ffn"), P("ffn", "mp"))
    return jax.shard_map(
        local, mesh=mesh, in_specs=placed, out_specs=P("ffn", "mp"), check_vma=False
    )
```
